32 devices in a mesh: rep: 8 (over y, x, core), sp: 4 (over z).
Axes of the slice: x: 2, y: 2, z: 4, core: 2. Of those that a mesh axis runs over, the one named last changes fastest.
Arguments:
- field: bfloat16 [8, 128, 100, 128], P('rep', 'sp'), may hold values from -6 to 6
- send_blocks: int32 [4, 4, 8], P('sp'), may hold values from 0 to 31
- send_count: int32 [4, 4], P('sp'), may hold values from 1 to 8, as said below
- regrid_weights: bfloat16 [32, 8, 128, 128], P('sp'), may hold values from -0.1875 to 0.1875
- tile_slot: int32 [32, 8], P('sp'), may hold values from 0 to 31
- edge_inputs: bfloat16 [12288, 1536], P(('rep', 'sp')), may hold values from -6 to 6
- cotangent: bfloat16 [12288, 512], P(('rep', 'sp')), may hold values from -0.15625 to 0.15625
Outputs:
- hidden: bfloat16 [8, 32, 100, 128], P('rep', 'sp')
- weight_grad: float32 [1536, 512], P(('rep', 'sp'))
The draws below stay inside these ranges and needn't reach their ends.
Inputs may be any that keep to these rules, and one draw needn't show every extreme that they name: `send_count`: every count is at most 8, and some pair of shards has exactly 8 in every draw.
All inputs are finite; a program needn't handle non-finite values.
Results may differ from the reference program's by a relative error of at most 0.001.
Values may be sent and summed in bfloat16 or wider, within the bound.
A program may use at most 64 MiB of HBM per device.

```python
import jax
import jax.numpy as jnp
from jax import lax

CHANNELS = 100
HID = 512
BLK = 128
NODE_TILE = 128
READS = 8
BLOCKS_DEV = 32
PER = 8
EDGE_DEV = 384
SHARDS = 4
REPLICAS = 8
BLOCKS = 128
TILES = 32
SLOTS = 32
IN = 1536
EDGES = 12288
N_REP = 8
N_SP = 4


def draw_send_count(key, part):
    base_key = jax.random.fold_in(key, 11)
    first_key, second_key = jax.random.split(base_key)
    counts = jax.random.randint(first_key, (SHARDS * SHARDS,), 1, PER + 1)
    chosen = jax.random.randint(second_key, (), 0, SHARDS * SHARDS)
    counts = jnp.where(jnp.arange(SHARDS * SHARDS) == chosen, PER, counts)
    return counts.reshape(SHARDS, SHARDS).astype(jnp.int32)


def with_ends(array, stream_key, smallest, largest):
    shape = array.shape
    place = [jax.random.randint(jax.random.fold_in(stream_key, axis), (), 0, shape[axis]) for axis in range(len(shape))]
    array = array.at[tuple(place)].set(smallest)
    longest = shape.index(max(shape))
    place[longest] = (place[longest] + 1) % shape[longest]
    return array.at[tuple(place)].set(largest)


def raised(entries, key, source, target, blocks, factor):
    def block_of(position):
        return (jnp.arange(entries.shape[position]) // (entries.shape[position] // blocks)).reshape((-1,) + (1,) * (entries.ndim - 1 - position))

    one_side = jax.random.permutation(key, blocks)[block_of(target)]
    second = (block_of(target) + blocks // 2) % blocks
    return jnp.where((block_of(source) == one_side) | (block_of(source) == second), factor * entries, entries)


def levels(key, dims, cuts, smallest, high):
    factor_of, own = 1.0, jax.random.fold_in(key, 6)
    for axis_at, shards_of in cuts:
        draws = jnp.exp(jax.random.uniform(jax.random.fold_in(own, axis_at), (shards_of,), jnp.float32, smallest / len(cuts), high / len(cuts)))
        factor_of = factor_of * jnp.repeat(draws, dims[axis_at] // shards_of).reshape([-1 if axis == axis_at else 1 for axis in range(len(dims))])
    return factor_of


def gaussian(key, dims, width, reach, cuts=(), kind=jnp.bfloat16):
    values = jax.random.normal(key, dims, jnp.float32) * width
    if len(cuts) > 0:
        values = levels(key, dims, cuts, -0.22, 0.18) * values
    return jnp.clip(values, min=-reach, max=reach).astype(kind)


def gaussian_with(rng, dims, scale, bound, cuts, heavy, kind=jnp.bfloat16):
    drawn = scale * jax.random.normal(rng, dims, jnp.float32)
    if cuts:
        drawn = drawn * levels(rng, dims, cuts, -0.22, 0.18)
    return jnp.clip(raised(drawn, jax.random.fold_in(rng, 3), *heavy), -bound, bound).astype(kind)


def setup_inputs(seed: int = 0) -> dict:
    key_of = jax.random.split(jax.random.key(seed), 8)
    return {
        "field": gaussian(key_of[0], (REPLICAS, BLOCKS, CHANNELS, BLK), 1.0, 6.0, ((0, 8), (1, 4))),
        "send_blocks": with_ends(jax.random.randint(key_of[1], (SHARDS, SHARDS, PER), 0, BLOCKS_DEV), jax.random.fold_in(key_of[1], 1), 0, BLOCKS_DEV - 1).astype(jnp.int32),
        "send_count": draw_send_count(jax.random.fold_in(key_of[7], 71), 0),
        "regrid_weights": gaussian(key_of[3], (TILES, READS, BLK, NODE_TILE), (READS * BLK) ** -0.5, 0.1875, ((0, 4),)),
        "tile_slot": with_ends(jax.random.randint(key_of[4], (TILES, READS), 0, SLOTS), jax.random.fold_in(key_of[4], 1), 0, SLOTS - 1).astype(jnp.int32),
        "edge_inputs": gaussian_with(key_of[5], (EDGES, IN), 1.0, 6.0, ((0, 32),), (0, 1, 32, 2.75)),
        "cotangent": gaussian(key_of[6], (EDGES, HID), (EDGE_DEV * N_SP) ** -0.5, 0.15625, ((0, 32),)),
    }


def reference(field, send_blocks, send_count, regrid_weights, tile_slot, edge_inputs, cotangent):
    shards = send_blocks.shape[0]
    slots_each = send_blocks.shape[2]
    blocks_dev = field.shape[1] // shards
    tiles_dev = tile_slot.shape[0] // shards
    reads = tile_slot.shape[1]
    source = jnp.arange(shards, dtype=jnp.int32)
    global_block = source[:, None, None] * blocks_dev + send_blocks
    alive_mask = jnp.arange(slots_each, dtype=jnp.int32)[None, None, :] < send_count[:, :, None]
    global_block = jnp.transpose(global_block, (1, 0, 2)).reshape(shards, shards * slots_each)
    alive_mask = jnp.transpose(alive_mask, (1, 0, 2)).reshape(shards, shards * slots_each)
    slot_index = tile_slot.reshape(shards, tiles_dev, reads)
    weight_tiles = regrid_weights.reshape(shards, tiles_dev, reads, BLK, NODE_TILE)

    def one_sample(sample):
        def one_shard(pieces):
            blocks_read, alive, slots, weights = pieces
            received = jnp.where(alive[:, None, None], sample[blocks_read], jnp.zeros((), jnp.bfloat16))
            picked = received[slots]
            result = jnp.einsum("tbcx,tbxn->tcn", picked.astype(jnp.float32), weights.astype(jnp.float32))
            return result.astype(jnp.bfloat16)

        outcome = lax.map(one_shard, (global_block, alive_mask, slot_index, weight_tiles))
        return outcome.reshape(shards * tiles_dev, CHANNELS, NODE_TILE)

    hidden = lax.map(one_sample, field)

    groups = N_REP * N_SP
    edge_groups = edge_inputs.reshape(groups, edge_inputs.shape[0] // groups, edge_inputs.shape[1])
    cot_groups = cotangent.reshape(groups, cotangent.shape[0] // groups, cotangent.shape[1])

    def accumulate(carry, pieces):
        left, right = pieces
        product = lax.dot_general(left, right, (((0,), (0,)), ((), ())), preferred_element_type=jnp.float32)
        return carry + product, None

    start_grad = jnp.zeros((edge_inputs.shape[1], cotangent.shape[1]), jnp.float32)
    weight_grad, unused = lax.scan(accumulate, start_grad, (edge_groups, cot_groups))
    return hidden, weight_grad
```

```python
import functools

import jax
import jax.numpy as jnp
from jax import lax
from jax.experimental import pallas as pl
from jax.experimental.pallas import tpu as pltpu
from jax.sharding import PartitionSpec as P

MESH = pl.DeviceIdType.MESH


def body(field, send_blocks, send_count, regrid_weights, tile_slot, edge_inputs, cotangent):
    sample = field[0]
    own_lists = send_blocks[0]
    shards = own_lists.shape[0]
    slots_each = own_lists.shape[1]
    channels = sample.shape[1]
    cells = sample.shape[2]
    alive = jnp.arange(slots_each, dtype=jnp.int32)[None, :] < send_count[0][:, None]
    outgoing = jnp.where(alive[:, :, None, None], sample[own_lists], jnp.zeros((), jnp.bfloat16))
    incoming = lax.all_to_all(outgoing, "sp", split_axis=0, concat_axis=0, tiled=True)
    block_pool = incoming.reshape(shards * slots_each, channels, cells)
    picked = block_pool[tile_slot]
    hidden = jnp.einsum(
        "tbcx,tbxn->tcn", picked, regrid_weights, preferred_element_type=jnp.float32
    )
    hidden = hidden.astype(jnp.bfloat16)[None]
    partial_value = lax.psum_scatter(
        lax.dot_general(
            edge_inputs, cotangent, (((0,), (0,)), ((), ())), preferred_element_type=jnp.float32
        ),
        "rep",
        scatter_dimension=0,
        tiled=True,
    )
    weight_grad = lax.psum_scatter(partial_value, "sp", scatter_dimension=0, tiled=True)
    return (hidden, weight_grad)


def kernel(
    n_sp, lists, counts, slots, field_hbm, weights_hbm, edge_hbm, cot_hbm,
    hidden_out, grad_out,
    field, weights, edge, cot, outgoing, pool, part, got1, got2, got3, gotz,
    load_sem, a2a_send, a2a_recv, s1, r1, s2, r2, s3, r3, sz, rz,
):
    rep = lax.axis_index("rep")
    me = lax.axis_index("sp")
    core = rep % 2
    x = (rep // 2) % 2
    y = rep // 4
    w1, w2 = 1 + core, 2 - core
    b1 = x + core * (y - x)
    b2 = y + core * (x - y)
    twin = rep + 1 - 2 * core
    first = rep + (1 - 2 * b1) * 2 * w1
    second = rep + (1 - 2 * b2) * 2 * w2
    blocks = field_hbm.shape[1]
    slots_each = lists.shape[2]
    tiles, reads = slots.shape
    width = edge_hbm.shape[1] // 4
    rows = part.shape[3]

    loads = [
        pltpu.make_async_copy(field_hbm.at[0], field.at[pl.ds(0, blocks)], load_sem.at[0]),
        pltpu.make_async_copy(edge_hbm, edge, load_sem.at[1]),
        pltpu.make_async_copy(cot_hbm, cot, load_sem.at[2]),
        pltpu.make_async_copy(weights_hbm, weights, load_sem.at[3]),
    ]
    for load in loads:
        load.start()

    barrier = pltpu.get_barrier_semaphore()
    sp_peers = [lax.rem(me + k, n_sp) for k in range(1, n_sp)]
    for peer in sp_peers:
        pl.semaphore_signal(barrier, inc=1, device_id=(rep, peer), device_id_type=MESH)
    for peer in (twin, first, second):
        pl.semaphore_signal(barrier, inc=1, device_id=(peer, me), device_id_type=MESH)

    field[blocks] = jnp.zeros(field.shape[1:], field.dtype)
    loads[0].wait()
    pl.semaphore_wait(barrier, n_sp - 1 + 3)

    def block_for(d, j):
        return field[jnp.where(j < counts[0, d], lists[0, d, j], blocks)]

    def send(src, dst, ssem, rsem, device):
        copy = pltpu.make_async_remote_copy(
            src_ref=src, dst_ref=dst, send_sem=ssem, recv_sem=rsem,
            device_id=device, device_id_type=MESH,
        )
        copy.start()
        return copy

    a2a = []
    for k in range(n_sp - 1):
        for j in range(slots_each):
            outgoing[k, j] = block_for(sp_peers[k], j)
        a2a.append(send(
            outgoing.at[k], pool.at[pl.ds(me * slots_each, slots_each)],
            a2a_send.at[k], a2a_recv.at[k], (rep, sp_peers[k]),
        ))

    def chunk(flip1, flip2):
        return (b1 + flip1 * (1 - 2 * b1)) * w1 + (b2 + flip2 * (1 - 2 * b2)) * w2

    loads[1].wait()
    loads[2].wait()
    to_twin = []
    for k, (f1, f2) in enumerate(((1, 1), (0, 1), (1, 0), (0, 0))):
        q = chunk(f1, f2)
        columns = pl.ds(pl.multiple_of(q * width, 128), width)
        value = lax.dot_general(
            edge[:, columns], cot[...], (((0,), (0,)), ((), ())),
            preferred_element_type=jnp.float32,
        )
        part[q] = value.reshape(part.shape[1:])
        to_twin.append(send(
            part.at[q, 1 - core], got1.at[k], s1.at[k], r1.at[k], (twin, me)
        ))
    for j in range(slots_each):
        pool[me * slots_each + j] = block_for(me, j)

    order = sp_peers + [me]
    c_both, c_first, c_second, c_none = chunk(1, 1), chunk(1, 0), chunk(0, 1), chunk(0, 0)

    def fold(q, k):
        to_twin[k].wait_recv()
        part[q, core] = part[q, core] + got1[k]

    out2 = []
    for k, q in enumerate((c_both, c_first)):
        fold(q, k)
        for i in range(n_sp):
            out2.append(send(
                part.at[q, core, order[i]], got2.at[k, order[i]],
                s2.at[k, i], r2.at[k, i], (first, me),
            ))
    fold(c_second, 2)
    fold(c_none, 3)
    out3 = []
    for i in range(n_sp):
        out2[i].wait_recv()
        part[c_second, core, order[i]] = part[c_second, core, order[i]] + got2[0, order[i]]
        out3.append(send(
            part.at[c_second, core, order[i]], got3.at[order[i]],
            s3.at[i], r3.at[i], (second, me),
        ))
    outz = []
    for i in range(n_sp):
        out2[n_sp + i].wait_recv()
        out3[i].wait_recv()
        total = part[c_none, core, order[i]] + got2[1, order[i]] + got3[order[i]]
        part[c_none, core, order[i]] = total
        if i < n_sp - 1:
            outz.append(send(
                part.at[c_none, core, order[i]], gotz.at[i], sz.at[i], rz.at[i], (rep, order[i])
            ))

    for copy in a2a:
        copy.wait_recv()
    loads[3].wait()
    for t in range(tiles):
        left = jnp.concatenate([pool[slots[t, b]] for b in range(reads)], axis=1)
        right = weights[t].reshape(reads * weights.shape[2], weights.shape[3])
        value = jnp.dot(left, right, preferred_element_type=jnp.float32)
        hidden_out[0, t] = value.astype(hidden_out.dtype)

    for copy in outz:
        copy.wait_recv()
    total = part[c_none, core, me]
    for i in range(n_sp - 1):
        total = total + gotz[i]
    grad_out[...] = total
    for copy in a2a + to_twin + out2 + out3 + outz:
        copy.wait_send()


def fused(mesh, field, send_blocks, send_count, regrid_weights, tile_slot, edge_inputs, cotangent):
    n_sp = mesh.shape["sp"]
    n_rep = mesh.shape["rep"]
    _, blocks, channels, cells = field.shape
    slots_each = send_blocks.shape[2]
    tiles = tile_slot.shape[0]
    n_in, hid = edge_inputs.shape[1], cotangent.shape[1]
    rows = n_in // (n_rep * n_sp)
    bf16, f32 = jnp.bfloat16, jnp.float32
    dma = pltpu.SemaphoreType.DMA
    smem = pl.BlockSpec(memory_space=pltpu.SMEM)
    far = pl.BlockSpec(memory_space=pl.ANY)
    near = pl.BlockSpec(memory_space=pltpu.VMEM)
    return pl.pallas_call(
        functools.partial(kernel, n_sp),
        out_shape=(
            jax.ShapeDtypeStruct((1, tiles, channels, regrid_weights.shape[3]), bf16),
            jax.ShapeDtypeStruct((rows, hid), f32),
        ),
        in_specs=[smem, smem, smem, far, far, far, far],
        out_specs=(near, near),
        scratch_shapes=[
            pltpu.VMEM((blocks + 1, channels, cells), bf16),
            pltpu.VMEM(regrid_weights.shape, bf16),
            pltpu.VMEM(edge_inputs.shape, bf16),
            pltpu.VMEM(cotangent.shape, bf16),
            pltpu.VMEM((n_sp - 1, slots_each, channels, cells), bf16),
            pltpu.VMEM((n_sp * slots_each, channels, cells), bf16),
            pltpu.VMEM((4, 2, n_sp, rows, hid), f32),
            pltpu.VMEM((4, n_sp, rows, hid), f32),
            pltpu.VMEM((2, n_sp, rows, hid), f32),
            pltpu.VMEM((n_sp, rows, hid), f32),
            pltpu.VMEM((n_sp - 1, rows, hid), f32),
            dma((4,)),
            dma((n_sp - 1,)), dma((n_sp - 1,)),
            dma((4,)), dma((4,)),
            dma((2, n_sp)), dma((2, n_sp)),
            dma((n_sp,)), dma((n_sp,)),
            dma((n_sp - 1,)), dma((n_sp - 1,)),
        ],
        compiler_params=pltpu.CompilerParams(
            collective_id=0, has_side_effects=True, vmem_limit_bytes=56 * 1024 * 1024
        ),
    )(send_blocks, send_count, tile_slot, field, regrid_weights, edge_inputs, cotangent)


def solution(mesh):
    in_specs = (
        P("rep", "sp", None, None),
        P("sp", None, None),
        P("sp", None),
        P("sp", None, None, None),
        P("sp", None),
        P(("rep", "sp"), None),
        P(("rep", "sp"), None),
    )
    out_specs = (P("rep", "sp", None, None), P(("rep", "sp"), None))
    binary = mesh.shape["rep"] == 2 * 2 * 2
    inner = functools.partial(fused, mesh) if binary else body
    return jax.shard_map(inner, mesh=mesh, in_specs=in_specs, out_specs=out_specs, check_vma=False)
```

```python
import jax
import jax.numpy as jnp
from jax import lax
from jax.experimental import pallas as pl
from jax.experimental.pallas import tpu as pltpu
from jax.sharding import PartitionSpec as P

MESH = pl.DeviceIdType.MESH


def body(field, send_blocks, send_count, regrid_weights, tile_slot, edge_inputs, cotangent):
    sample = field[0]
    own_lists = send_blocks[0]
    shards = own_lists.shape[0]
    slots_each = own_lists.shape[1]
    channels = sample.shape[1]
    cells = sample.shape[2]
    alive = jnp.arange(slots_each, dtype=jnp.int32)[None, :] < send_count[0][:, None]
    outgoing = jnp.where(alive[:, :, None, None], sample[own_lists], jnp.zeros((), jnp.bfloat16))
    incoming = lax.all_to_all(outgoing, "sp", split_axis=0, concat_axis=0, tiled=True)
    block_pool = incoming.reshape(shards * slots_each, channels, cells)
    picked = block_pool[tile_slot]
    hidden = jnp.einsum(
        "tbcx,tbxn->tcn", picked, regrid_weights, preferred_element_type=jnp.float32
    )
    hidden = hidden.astype(jnp.bfloat16)[None]
    partial_value = lax.psum_scatter(
        lax.dot_general(
            edge_inputs, cotangent, (((0,), (0,)), ((), ())), preferred_element_type=jnp.float32
        ),
        "rep",
        scatter_dimension=0,
        tiled=True,
    )
    weight_grad = lax.psum_scatter(partial_value, "sp", scatter_dimension=0, tiled=True)
    return (hidden, weight_grad)


def kernel(
    lists, counts, slots, field_hbm, weights_hbm, edge_hbm, cot_hbm,
    hidden_out, grad_out,
    field, wide, weights, edge, cot, outgoing, pool, tall, part, got1, got2, got3, gotz, gotf,
    load_sem, a2a_send, a2a_recv, s1, r1, s2, r2, s3, r3, sz, rz, sf, rf,
):
    rep = lax.axis_index("rep")
    me = lax.axis_index("sp")
    core = rep % 2
    x = (rep // 2) % 2
    y = rep // 4
    w1, w2 = 1 + core, 2 - core
    b1 = x + core * (y - x)
    b2 = y + core * (x - y)
    twin = rep + 1 - 2 * core
    first = rep + (1 - 2 * b1) * 2 * w1
    second = rep + (1 - 2 * b2) * 2 * w2
    low, high = me % 2, me // 2
    near = 2 * high + 1 - low
    far = 2 * (1 - high) + low
    diag = 2 * (1 - high) + 1 - low
    channels, blocks, cells = field.shape
    slots_each = lists.shape[2]
    tiles, reads = slots.shape
    width = edge_hbm.shape[1] // 4

    loads = [
        pltpu.make_async_copy(field_hbm.at[0], field, load_sem.at[0]),
        pltpu.make_async_copy(edge_hbm, edge, load_sem.at[1]),
        pltpu.make_async_copy(cot_hbm, cot, load_sem.at[2]),
        pltpu.make_async_copy(weights_hbm, weights, load_sem.at[3]),
    ]
    for load in loads:
        load.start()

    barrier = pltpu.get_barrier_semaphore()
    sp_peers = [far, diag, near]
    for peer in sp_peers:
        pl.semaphore_signal(barrier, inc=1, device_id=(rep, peer), device_id_type=MESH)
    for peer in (twin, first, second):
        pl.semaphore_signal(barrier, inc=1, device_id=(peer, me), device_id_type=MESH)

    loads[0].wait()
    wide[...] = field[...].astype(jnp.float32).reshape(wide.shape)

    def block_for(d, j):
        block = wide[pl.ds(lists[0, d, j], channels, stride=blocks), :]
        block = jnp.where(j < counts[0, d], block, jnp.zeros_like(block))
        return block.astype(jnp.bfloat16)

    def send(src, dst, ssem, rsem, device):
        copy = pltpu.make_async_remote_copy(
            src_ref=src, dst_ref=dst, send_sem=ssem, recv_sem=rsem,
            device_id=device, device_id_type=MESH,
        )
        copy.start()
        return copy

    a2a = []
    for k, peer in enumerate(sp_peers):
        for j in range(slots_each):
            outgoing[k, j] = block_for(peer, j)
        if k == 0:
            pl.semaphore_wait(barrier, 6)
        a2a.append(send(
            outgoing.at[k], pool.at[pl.ds(me * slots_each, slots_each)],
            a2a_send.at[k], a2a_recv.at[k], (rep, peer),
        ))

    def chunk(flip1, flip2):
        return (b1 + flip1 * (1 - 2 * b1)) * w1 + (b2 + flip2 * (1 - 2 * b2)) * w2

    loads[1].wait()
    loads[2].wait()
    to_twin = []
    for k, (f1, f2) in enumerate(((1, 1), (0, 1), (1, 0), (0, 0))):
        q = chunk(f1, f2)
        columns = pl.ds(pl.multiple_of(q * width, 128), width)
        value = lax.dot_general(
            edge[:, columns], cot[...], (((0,), (0,)), ((), ())),
            preferred_element_type=jnp.float32,
        )
        part[q] = value.reshape(part.shape[1:])
        to_twin.append(send(
            part.at[q, 1 - core], got1.at[k], s1.at[k], r1.at[k], (twin, me)
        ))
    for j in range(slots_each):
        pool[me * slots_each + j] = block_for(me, j)

    order = [diag, near, far, me]
    c_both, c_first, c_second, c_none = chunk(1, 1), chunk(1, 0), chunk(0, 1), chunk(0, 0)

    def fold(q, k):
        to_twin[k].wait_recv()
        part[q, core] = part[q, core] + got1[k]

    out2 = []
    for k, q in enumerate((c_both, c_first)):
        fold(q, k)
        for i in range(4):
            out2.append(send(
                part.at[q, core, order[i]], got2.at[k, order[i]],
                s2.at[k, i], r2.at[k, i], (first, me),
            ))
    fold(c_second, 2)
    fold(c_none, 3)
    out3 = []
    for i in range(4):
        out2[i].wait_recv()
        part[c_second, core, order[i]] = part[c_second, core, order[i]] + got2[0, order[i]]
        out3.append(send(
            part.at[c_second, core, order[i]], got3.at[order[i]],
            s3.at[i], r3.at[i], (second, me),
        ))
    outz = []
    for i in range(4):
        out2[4 + i].wait_recv()
        out3[i].wait_recv()
        total = part[c_none, core, order[i]] + got2[1, order[i]] + got3[order[i]]
        part[c_none, core, order[i]] = total
        if i < 2:
            outz.append(send(
                part.at[c_none, core, order[i]], gotz.at[i], sz.at[i], rz.at[i], (rep, near)
            ))
    outz[0].wait_recv()
    part[c_none, core, far] = part[c_none, core, far] + gotz[0]
    last = send(part.at[c_none, core, far], gotf, sf, rf, (rep, far))

    for copy in a2a:
        copy.wait_recv()
    loads[3].wait()
    for t in range(tiles):
        left = jnp.concatenate([pool[slots[t, b]] for b in range(reads)], axis=1)
        right = weights[t].reshape(reads * weights.shape[2], weights.shape[3])
        tall[pl.ds(t, channels, stride=tiles), :] = jnp.dot(
            left, right, preferred_element_type=jnp.float32
        )
    hidden_out[0] = tall[...].reshape(hidden_out.shape[1:]).astype(hidden_out.dtype)

    outz[1].wait_recv()
    total = part[c_none, core, me] + gotz[1]
    last.wait_recv()
    grad_out[...] = total + gotf[...]
    for copy in a2a + to_twin + out2 + out3 + outz + [last]:
        copy.wait_send()


def settle(hidden, grad, hidden_out, grad_out):
    hidden_out[...] = hidden[...]
    grad_out[...] = grad[...]


def fused(field, send_blocks, send_count, regrid_weights, tile_slot, edge_inputs, cotangent):
    _, blocks, channels, cells = field.shape
    slots_each = send_blocks.shape[2]
    tiles = tile_slot.shape[0]
    nodes = regrid_weights.shape[3]
    n_in, hid = edge_inputs.shape[1], cotangent.shape[1]
    rows = n_in // (lax.axis_size("rep") * lax.axis_size("sp"))
    bf16, f32 = jnp.bfloat16, jnp.float32
    dma = pltpu.SemaphoreType.DMA
    smem = pl.BlockSpec(memory_space=pltpu.SMEM)
    far = pl.BlockSpec(memory_space=pl.ANY)
    near = pl.BlockSpec(memory_space=pltpu.VMEM)
    out_shape = (
        jax.ShapeDtypeStruct((1, channels, tiles, nodes), bf16),
        jax.ShapeDtypeStruct((rows, hid), f32),
    )
    hidden, grad = pl.pallas_call(
        kernel,
        out_shape=out_shape,
        in_specs=[smem, smem, smem, far, far, far, far],
        out_specs=(near, near),
        scratch_shapes=[
            pltpu.VMEM((channels, blocks, cells), bf16),
            pltpu.VMEM((channels * blocks, cells), f32),
            pltpu.VMEM(regrid_weights.shape, bf16),
            pltpu.VMEM(edge_inputs.shape, bf16),
            pltpu.VMEM(cotangent.shape, bf16),
            pltpu.VMEM((3, slots_each, channels, cells), bf16),
            pltpu.VMEM((4 * slots_each, channels, cells), bf16),
            pltpu.VMEM((channels * tiles, nodes), f32),
            pltpu.VMEM((4, 2, 4, rows, hid), f32),
            pltpu.VMEM((4, 4, rows, hid), f32),
            pltpu.VMEM((2, 4, rows, hid), f32),
            pltpu.VMEM((4, rows, hid), f32),
            pltpu.VMEM((2, rows, hid), f32),
            pltpu.VMEM((rows, hid), f32),
            dma((4,)),
            dma((3,)), dma((3,)),
            dma((4,)), dma((4,)),
            dma((2, 4)), dma((2, 4)),
            dma((4,)), dma((4,)),
            dma((2,)), dma((2,)),
            dma, dma,
        ],
        compiler_params=pltpu.CompilerParams(
            collective_id=0, has_side_effects=True, vmem_limit_bytes=56 * 1024 * 1024
        ),
    )(
        send_blocks, send_count, tile_slot, jnp.transpose(field, (0, 2, 1, 3)),
        regrid_weights, edge_inputs, cotangent,
    )
    hidden, grad = pl.pallas_call(
        settle, out_shape=out_shape, in_specs=[near, near], out_specs=(near, near),
        compiler_params=pltpu.CompilerParams(vmem_limit_bytes=4 * 1024 * 1024),
    )(hidden, grad)
    return jnp.transpose(hidden, (0, 2, 1, 3)), grad


def solution(mesh):
    in_specs = (
        P("rep", "sp", None, None),
        P("sp", None, None),
        P("sp", None),
        P("sp", None, None, None),
        P("sp", None),
        P(("rep", "sp"), None),
        P(("rep", "sp"), None),
    )
    out_specs = (P("rep", "sp", None, None), P(("rep", "sp"), None))
    binary = mesh.shape["rep"] == 2 * 2 * 2 and mesh.shape["sp"] == 2 * 2
    inner = fused if binary else body
    return jax.shard_map(inner, mesh=mesh, in_specs=in_specs, out_specs=out_specs, check_vma=False)
```

```python
import jax
import jax.numpy as jnp
from jax import lax
from jax.experimental import pallas as pl
from jax.experimental.pallas import tpu as pltpu
from jax.sharding import PartitionSpec as P

MESH = pl.DeviceIdType.MESH


def body(field, send_blocks, send_count, regrid_weights, tile_slot, edge_inputs, cotangent):
    sample = field[0]
    own_lists = send_blocks[0]
    shards = own_lists.shape[0]
    slots_each = own_lists.shape[1]
    channels = sample.shape[1]
    cells = sample.shape[2]
    alive = jnp.arange(slots_each, dtype=jnp.int32)[None, :] < send_count[0][:, None]
    outgoing = jnp.where(alive[:, :, None, None], sample[own_lists], jnp.zeros((), jnp.bfloat16))
    incoming = lax.all_to_all(outgoing, "sp", split_axis=0, concat_axis=0, tiled=True)
    block_pool = incoming.reshape(shards * slots_each, channels, cells)
    picked = block_pool[tile_slot]
    hidden = jnp.einsum(
        "tbcx,tbxn->tcn", picked, regrid_weights, preferred_element_type=jnp.float32
    )
    hidden = hidden.astype(jnp.bfloat16)[None]
    partial_value = lax.psum_scatter(
        lax.dot_general(
            edge_inputs, cotangent, (((0,), (0,)), ((), ())), preferred_element_type=jnp.float32
        ),
        "rep",
        scatter_dimension=0,
        tiled=True,
    )
    weight_grad = lax.psum_scatter(partial_value, "sp", scatter_dimension=0, tiled=True)
    return (hidden, weight_grad)


def kernel(
    lists, counts, slots, field_hbm, weights_hbm, edge_hbm, cot_hbm,
    hidden_out, grad_out,
    field, wide, weights, edge, cot, outgoing, pool, tall, part, got1, got2, got3, gotz, gotf,
    load_sem, a2a_send, a2a_recv, s1, r1, s2, r2, s3, r3, sz, rz, sf, rf,
):
    rep = lax.axis_index("rep")
    me = lax.axis_index("sp")
    core = rep % 2
    x = (rep // 2) % 2
    y = rep // 4
    w1, w2 = 1 + core, 2 - core
    b1 = x + core * (y - x)
    b2 = y + core * (x - y)
    twin = rep + 1 - 2 * core
    first = rep + (1 - 2 * b1) * 2 * w1
    second = rep + (1 - 2 * b2) * 2 * w2
    low, high = me % 2, me // 2
    near = 2 * high + 1 - low
    far = 2 * (1 - high) + low
    diag = 2 * (1 - high) + 1 - low
    channels, blocks, cells = field.shape
    slots_each = lists.shape[2]
    tiles, reads = slots.shape
    width = edge_hbm.shape[1] // 4

    loads = [
        pltpu.make_async_copy(field_hbm.at[0], field, load_sem.at[0]),
        pltpu.make_async_copy(edge_hbm, edge, load_sem.at[1]),
        pltpu.make_async_copy(cot_hbm, cot, load_sem.at[2]),
        pltpu.make_async_copy(weights_hbm, weights, load_sem.at[3]),
    ]
    for i in (1, 2, 0, 3):
        loads[i].start()

    barrier = pltpu.get_barrier_semaphore()
    sp_peers = [far, diag, near]
    for peer in sp_peers:
        pl.semaphore_signal(barrier, inc=1, device_id=(rep, peer), device_id_type=MESH)
    for peer in (twin, first, second):
        pl.semaphore_signal(barrier, inc=1, device_id=(peer, me), device_id_type=MESH)

    def send(src, dst, ssem, rsem, device):
        copy = pltpu.make_async_remote_copy(
            src_ref=src, dst_ref=dst, send_sem=ssem, recv_sem=rsem,
            device_id=device, device_id_type=MESH,
        )
        copy.start()
        return copy

    def chunk(flip1, flip2):
        return (b1 + flip1 * (1 - 2 * b1)) * w1 + (b2 + flip2 * (1 - 2 * b2)) * w2

    c_both, c_first, c_second, c_none = chunk(1, 1), chunk(1, 0), chunk(0, 1), chunk(0, 0)
    order = [diag, far, near, me]
    to_twin, out2, out3, a2a = [], [], [], []

    def product(k, q):
        columns = pl.ds(pl.multiple_of(q * width, 128), width)
        value = lax.dot_general(
            edge[:, columns], cot[...], (((0,), (0,)), ((), ())),
            preferred_element_type=jnp.float32,
        )
        part[q] = value.reshape(part.shape[1:])
        if k == 0:
            pl.semaphore_wait(barrier, 6)
        to_twin.append(send(
            part.at[q, 1 - core], got1.at[k], s1.at[k], r1.at[k], (twin, me)
        ))

    def block_for(d, j):
        block = wide[pl.ds(lists[0, d, j], channels, stride=blocks), :]
        block = jnp.where(j < counts[0, d], block, jnp.zeros_like(block))
        return block.astype(jnp.bfloat16)

    def send_blocks_to(k):
        peer = sp_peers[k]
        for j in range(slots_each):
            outgoing[k, j] = block_for(peer, j)
        a2a.append(send(
            outgoing.at[k], pool.at[pl.ds(me * slots_each, slots_each)],
            a2a_send.at[k], a2a_recv.at[k], (rep, peer),
        ))

    def fold(q, k):
        to_twin[k].wait_recv()
        part[q, core] = part[q, core] + got1[k]

    def send_first(k, q):
        fold(q, k)
        for i in range(4):
            out2.append(send(
                part.at[q, core, order[i]], got2.at[k, order[i]],
                s2.at[k, i], r2.at[k, i], (first, me),
            ))

    loads[1].wait()
    loads[2].wait()
    product(0, c_both)
    product(1, c_second)
    loads[0].wait()
    wide[...] = field[...].astype(jnp.float32).reshape(wide.shape)
    send_blocks_to(0)
    send_first(0, c_both)
    product(2, c_first)
    send_blocks_to(1)
    send_first(1, c_first)
    send_blocks_to(2)
    product(3, c_none)
    for j in range(slots_each):
        pool[me * slots_each + j] = block_for(me, j)
    fold(c_second, 2)
    fold(c_none, 3)
    for i in range(4):
        out2[i].wait_recv()
        part[c_second, core, order[i]] = part[c_second, core, order[i]] + got2[0, order[i]]
        out3.append(send(
            part.at[c_second, core, order[i]], got3.at[order[i]],
            s3.at[i], r3.at[i], (second, me),
        ))
    outz = []
    for i in range(4):
        out2[4 + i].wait_recv()
        out3[i].wait_recv()
        total = part[c_none, core, order[i]] + got2[1, order[i]] + got3[order[i]]
        part[c_none, core, order[i]] = total
        if i in (0, 2):
            k = len(outz)
            outz.append(send(
                part.at[c_none, core, order[i]], gotz.at[k], sz.at[k], rz.at[k], (rep, near)
            ))
        if i == 2:
            outz[0].wait_recv()
            part[c_none, core, far] = part[c_none, core, far] + gotz[0]
            last = send(part.at[c_none, core, far], gotf, sf, rf, (rep, far))

    for copy in a2a:
        copy.wait_recv()
    loads[3].wait()
    for t in range(tiles):
        left = jnp.concatenate([pool[slots[t, b]] for b in range(reads)], axis=1)
        right = weights[t].reshape(reads * weights.shape[2], weights.shape[3])
        tall[pl.ds(t, channels, stride=tiles), :] = jnp.dot(
            left, right, preferred_element_type=jnp.float32
        )
    hidden_out[0] = tall[...].reshape(hidden_out.shape[1:]).astype(hidden_out.dtype)

    outz[1].wait_recv()
    total = part[c_none, core, me] + gotz[1]
    last.wait_recv()
    grad_out[...] = total + gotf[...]
    for copy in a2a + to_twin + out2 + out3 + outz + [last]:
        copy.wait_send()


def settle(hidden, grad, hidden_out, grad_out):
    hidden_out[...] = hidden[...]
    grad_out[...] = grad[...]


def fused(field, send_blocks, send_count, regrid_weights, tile_slot, edge_inputs, cotangent):
    _, blocks, channels, cells = field.shape
    slots_each = send_blocks.shape[2]
    tiles = tile_slot.shape[0]
    nodes = regrid_weights.shape[3]
    n_in, hid = edge_inputs.shape[1], cotangent.shape[1]
    rows = n_in // (lax.axis_size("rep") * lax.axis_size("sp"))
    bf16, f32 = jnp.bfloat16, jnp.float32
    dma = pltpu.SemaphoreType.DMA
    smem = pl.BlockSpec(memory_space=pltpu.SMEM)
    far = pl.BlockSpec(memory_space=pl.ANY)
    near = pl.BlockSpec(memory_space=pltpu.VMEM)
    out_shape = (
        jax.ShapeDtypeStruct((1, channels, tiles, nodes), bf16),
        jax.ShapeDtypeStruct((rows, hid), f32),
    )
    hidden, grad = pl.pallas_call(
        kernel,
        out_shape=out_shape,
        in_specs=[smem, smem, smem, far, far, far, far],
        out_specs=(near, near),
        scratch_shapes=[
            pltpu.VMEM((channels, blocks, cells), bf16),
            pltpu.VMEM((channels * blocks, cells), f32),
            pltpu.VMEM(regrid_weights.shape, bf16),
            pltpu.VMEM(edge_inputs.shape, bf16),
            pltpu.VMEM(cotangent.shape, bf16),
            pltpu.VMEM((3, slots_each, channels, cells), bf16),
            pltpu.VMEM((4 * slots_each, channels, cells), bf16),
            pltpu.VMEM((channels * tiles, nodes), f32),
            pltpu.VMEM((4, 2, 4, rows, hid), f32),
            pltpu.VMEM((4, 4, rows, hid), f32),
            pltpu.VMEM((2, 4, rows, hid), f32),
            pltpu.VMEM((4, rows, hid), f32),
            pltpu.VMEM((2, rows, hid), f32),
            pltpu.VMEM((rows, hid), f32),
            dma((4,)),
            dma((3,)), dma((3,)),
            dma((4,)), dma((4,)),
            dma((2, 4)), dma((2, 4)),
            dma((4,)), dma((4,)),
            dma((2,)), dma((2,)),
            dma, dma,
        ],
        compiler_params=pltpu.CompilerParams(
            collective_id=0, has_side_effects=True, vmem_limit_bytes=56 * 1024 * 1024
        ),
    )(
        send_blocks, send_count, tile_slot, jnp.transpose(field, (0, 2, 1, 3)),
        regrid_weights, edge_inputs, cotangent,
    )
    hidden, grad = pl.pallas_call(
        settle, out_shape=out_shape, in_specs=[near, near], out_specs=(near, near),
        compiler_params=pltpu.CompilerParams(vmem_limit_bytes=4 * 1024 * 1024),
    )(hidden, grad)
    return jnp.transpose(hidden, (0, 2, 1, 3)), grad


def solution(mesh):
    in_specs = (
        P("rep", "sp", None, None),
        P("sp", None, None),
        P("sp", None),
        P("sp", None, None, None),
        P("sp", None),
        P(("rep", "sp"), None),
        P(("rep", "sp"), None),
    )
    out_specs = (P("rep", "sp", None, None), P(("rep", "sp"), None))
    binary = mesh.shape["rep"] == 2 * 2 * 2 and mesh.shape["sp"] == 2 * 2
    inner = fused if binary else body
    return jax.shard_map(inner, mesh=mesh, in_specs=in_specs, out_specs=out_specs, check_vma=False)
```
